32 devices in a mesh: dp: 8 (over y, x, core), seq: 4 (over z).
Axes of the slice: x: 2, y: 2, z: 4, core: 2. Of those that a mesh axis runs over, the one named last changes fastest.
Arguments:
- tokens: bfloat16 [8, 512, 2048], P('dp', 'seq'), may hold values from -6 to 6
- qkv_weight: bfloat16 [3, 2048, 1024], P(None, 'dp', 'seq'), may hold values from -0.125 to 0.125
- qk_scale: float32 [1024], replicated, may hold values from 0.5 to 10
- out_weight: bfloat16 [1024, 2048], P('seq', 'dp'), may hold values from -0.1875 to 0.1875
- mix_rates: float32 [2, 2048], replicated, may hold values from 0.1 to 0.6
- gate_up_weight: bfloat16 [2, 2048, 8192], P(None, 'dp', 'seq'), may hold values from -0.125 to 0.125
- mlp_scales: float32 [2, 8192], P(None, 'seq'), may hold values from 0.5 to 2
- down_weight: bfloat16 [8192, 2048], P('seq', 'dp'), may hold values from -0.0625 to 0.0625
Outputs:
- result: bfloat16 [8, 512, 2048], P('dp', 'seq')
The draws below stay inside these ranges and needn't reach their ends.
All inputs are finite; a program needn't handle non-finite values.
Results may differ from the reference program's by a relative error of at most 0.015.
The reference program's roundings to bfloat16 on the way (of `normed`, `shares`, `attended`, `middle` and `hidden`) count: a program that leaves them out, or rounds other values in their place, can miss the bound.
Values may be sent and summed in bfloat16 or wider, within the bound.
No kernel may reach another device: no remote copies, remote signals or barrier semaphores. Data moves between devices by JAX's collectives and lax.ppermute only.
A program may use at most 128 MiB of HBM per device.

```python
import math
import jax
import jax.numpy as jnp
from jax import lax

D = 2048
H = 8
HD = 128
FF = 8192
LEN = 512
SEQS = 8


def draw_qk_scale(key, part):
    low_end, high_end = (0.5, 2.0)
    uniform_draw = jax.random.uniform(key, (H * HD,), jnp.float32)
    return jnp.exp(jnp.log(low_end) + uniform_draw * (jnp.log(high_end) - jnp.log(low_end)))


def level_of(own_key, extent, shards, low, largest):
    def one(position, parts):
        steps = jax.random.uniform(jax.random.fold_in(jax.random.fold_in(own_key, 6), position), (parts,), jnp.float32, low / len(shards), largest / len(shards))
        return jnp.repeat(jnp.exp(steps), extent[position] // parts).reshape((-1,) + (1,) * (len(extent) - position - 1))

    level = one(*shards[0])
    for cut in shards[1:]:
        level = level * one(*cut)
    return level


def scatter_about(rng, dims, width, bound, shards=(), kind=jnp.bfloat16):
    values = width * jax.random.normal(rng, dims, jnp.float32)
    if shards:
        values = values * level_of(rng, dims, shards, -0.22, 0.18)
    return jnp.clip(values, -bound, bound).astype(kind)


def setup_inputs(seed: int = 0) -> dict:
    arg_keys = jax.random.split(jax.random.key(seed), 9)
    tokens = scatter_about(arg_keys[0], (SEQS, LEN, D), 1.0, 6.0, ((0, 8), (1, 4)))
    qkv_weight = scatter_about(arg_keys[1], (3, D, H * HD), D ** -0.5, 0.125, ((1, 8), (2, 4)))
    qk_scale = draw_qk_scale(jax.random.fold_in(arg_keys[8], 71), 0)
    out_weight = scatter_about(arg_keys[3], (H * HD, D), (H * HD) ** -0.5, 0.1875, ((0, 4), (1, 8)))
    mix_rates = jnp.clip(jnp.exp(jax.random.uniform(arg_keys[4], (2, D), jnp.float32, math.log(0.1), math.log(0.6))), 0.1, 0.6)
    gate_up_weight = scatter_about(arg_keys[5], (2, D, FF), D ** -0.5, 0.125, ((1, 8), (2, 4)))
    mlp_scales = jnp.clip(jnp.exp(math.log(2.0) - 1.3862944 * jax.random.uniform(arg_keys[6], (2, FF), jnp.float32) ** level_of(arg_keys[6], (2, FF), ((1, 4),), -0.2, 0.2)), 0.5, 2.0)
    down_weight = scatter_about(arg_keys[7], (FF, D), FF ** -0.5, 0.0625, ((0, 4), (1, 8)))
    return {"tokens": tokens, "qkv_weight": qkv_weight, "qk_scale": qk_scale, "out_weight": out_weight, "mix_rates": mix_rates, "gate_up_weight": gate_up_weight, "mlp_scales": mlp_scales, "down_weight": down_weight}


def unit_rms(values_in):
    return values_in * lax.rsqrt(lax.optimization_barrier(jnp.mean(values_in * values_in, axis=-1, keepdims=True)) + 1e-06)

def prepare(projected, scale_heads):
    queries = unit_rms(projected[:, 0]) * scale_heads
    key_rows = unit_rms(projected[:, 1]) * scale_heads
    return jnp.stack([queries, key_rows, projected[:, 2]], axis=1).astype(jnp.bfloat16)

def attend(stacked):
    length = stacked.shape[0]
    head_count = stacked.shape[2]
    head_dim = stacked.shape[3]
    block_rows = min(length, 512)
    block_count = length // block_rows
    key_rows = stacked[:, 1].astype(jnp.float32)
    value_rows = stacked[:, 2].astype(jnp.float32)
    queries = stacked[:, 0].reshape(block_count, block_rows, head_count, head_dim)
    positions = jnp.arange(length, dtype=jnp.int32)
    factor = head_dim ** (-0.5)

    def one_block(inputs):
        block_index, query_block = inputs
        scores = jnp.einsum('qhd,khd->hqk', query_block.astype(jnp.float32), key_rows, precision=lax.Precision.HIGHEST) * factor
        query_pos = block_index * block_rows + jnp.arange(block_rows, dtype=jnp.int32)
        allowed = positions[None, :] <= query_pos[:, None]
        scores = jnp.where(allowed[None], scores, -1e+30)
        highest = lax.optimization_barrier(jnp.max(scores, axis=-1, keepdims=True))
        powers = jnp.exp(scores - highest)
        shares = (powers / lax.optimization_barrier(jnp.sum(powers, axis=-1, keepdims=True))).astype(jnp.bfloat16)
        mixed = jnp.einsum('hqk,khd->qhd', shares.astype(jnp.float32), value_rows, precision=lax.Precision.HIGHEST)
        return mixed.astype(jnp.bfloat16)
    mixed_all = lax.map(one_block, (jnp.arange(block_count, dtype=jnp.int32), queries))
    return mixed_all.reshape(length, head_count, head_dim)

def reference(tokens, qkv_weight, qk_scale, out_weight, mix_rates, gate_up_weight, mlp_scales, down_weight):
    scale_all = qk_scale.reshape(H, HD)

    def one_layer(own_rows):
        length = own_rows.shape[0]
        normed = unit_rms(own_rows.astype(jnp.float32)).astype(jnp.bfloat16)
        projected = jnp.einsum('td,cdn->tcn', normed.astype(jnp.float32), qkv_weight.astype(jnp.float32), precision=lax.Precision.HIGHEST)
        stacked = prepare(projected.reshape(length, 3, H, HD), scale_all)
        attended = attend(stacked).reshape(length, H * HD)
        attention = jnp.dot(attended, out_weight, preferred_element_type=jnp.float32)
        normed_f = normed.astype(jnp.float32)
        middle = unit_rms(normed_f + mix_rates[0] * (unit_rms(attention) - normed_f)).astype(jnp.bfloat16)
        gate_up = jnp.einsum('td,cdf->tcf', middle.astype(jnp.float32), gate_up_weight.astype(jnp.float32), precision=lax.Precision.HIGHEST)
        hidden = (jax.nn.silu(gate_up[:, 0] * mlp_scales[0]) * (gate_up[:, 1] * mlp_scales[1])).astype(jnp.bfloat16)
        feed_out = jnp.dot(hidden, down_weight, preferred_element_type=jnp.float32)
        middle_f = middle.astype(jnp.float32)
        return unit_rms(middle_f + mix_rates[1] * (unit_rms(feed_out) - middle_f)).astype(jnp.bfloat16)
    return lax.map(one_layer, tokens)
```

```python
import functools

import jax
import jax.numpy as jnp
from jax import lax
from jax.experimental import pallas as pl
from jax.experimental.pallas import tpu as pltpu
from jax.sharding import PartitionSpec as P

HD = 128
EPS = 1e-06
BF16 = jnp.bfloat16
F32 = jnp.float32


def hbm():
    return pl.BlockSpec(memory_space=pltpu.HBM)


def call(body, name, outs, scratch, flops, bytes_accessed, args):
    return pl.pallas_call(
        body,
        name=name,
        out_shape=outs,
        in_specs=[hbm()] * len(args),
        out_specs=jax.tree.map(lambda _: hbm(), outs),
        scratch_shapes=scratch,
        cost_estimate=pl.CostEstimate(flops=flops, bytes_accessed=bytes_accessed, transcendentals=0),
    )(*args)


def unit(v):
    return v * lax.rsqrt(jnp.mean(v * v, axis=-1, keepdims=True) + EPS)


def at(index, size):
    return pl.ds(pl.multiple_of(index * size, size), size)


def flip(array, axis, bit, size):
    return lax.ppermute(array, axis, [(i, i ^ bit) for i in range(size)])


def high_bit(k):
    return 1 << (k.bit_length() - 1)


def gather_line(own, axis, size):
    got = [own]
    for k in range(1, size):
        bit = high_bit(k)
        got.append(flip(got[k ^ bit], axis, bit, size))
    return got


def gather_plane(own, axis, size, split):
    upper = [k for k in range(0, size, 2)]
    got = {0: (own,)}
    for k in upper[1:]:
        high, low = high_bit(k), k & -k
        if high == low:
            got[k] = tuple(flip(p, axis, high, size) for p in got[0])
        elif split is None:
            got[k] = tuple(flip(p, axis, high, size) for p in got[k ^ high])
        else:
            first, second = got[k ^ high], got[k ^ low]
            first = first[0] if len(first) == 2 else split(first[0])[0]
            second = second[1] if len(second) == 2 else split(second[0])[1]
            got[k] = (flip(first, axis, high, size), flip(second, axis, low, size))
    for k in upper:
        got[k + 1] = tuple(flip(p, axis, 1, size) for p in got[k])
    return [got[k] for k in range(size)]


def qkv_attend(tokens, pieces, scale_all, dp, seq):
    rows, width = tokens[0].shape
    length = rows * seq
    _, part, cols = pieces[0].shape
    heads = cols // HD

    def body(*refs):
        tok_refs = refs[:seq]
        piece_refs = refs[seq : seq + dp]
        scale_ref = refs[seq + dp]
        normed_out, attended_out = refs[seq + dp + 1 : seq + dp + 3]
        tok_v, w_v, normed_v, proj_v, att_v, scale_v, tok_sem, w_sem, s_sem, n_sem, a_sem = refs[seq + dp + 3 :]
        d, z = lax.axis_index("dp"), lax.axis_index("seq")
        tok_copies = [
            pltpu.make_async_copy(tok_refs[j], tok_v.at[j], tok_sem.at[j]) for j in range(seq)
        ]
        w_copies = [
            pltpu.make_async_copy(piece_refs[k], w_v.at[:, at(d ^ k, part), :], w_sem.at[k])
            for k in range(dp)
        ]
        s_copy = pltpu.make_async_copy(scale_ref, scale_v, s_sem)
        for c in tok_copies + w_copies + [s_copy]:
            c.start()
        for j in range(seq):
            tok_copies[j].wait()
            normed_v[at(z ^ j, rows), :] = unit(tok_v[j].astype(F32)).astype(BF16)
        n_copy = pltpu.make_async_copy(normed_v, normed_out, n_sem)
        n_copy.start()
        for c in w_copies:
            c.wait()
        s_copy.wait()
        for c in range(3):
            proj = jnp.dot(normed_v[...], w_v[c], preferred_element_type=F32)
            for h in range(heads):
                one = proj[:, h * HD : (h + 1) * HD]
                if c < 2:
                    one = unit(one) * scale_v[pl.ds(z * heads + h, 1), :]
                proj_v[c, h] = one.astype(BF16)
        for h in range(heads):
            for i in range(seq):
                keys = (i + 1) * rows
                scores = (
                    lax.dot_general(
                        proj_v[0, h, i * rows : keys, :],
                        proj_v[1, h, :keys, :],
                        (((1,), (1,)), ((), ())),
                        preferred_element_type=F32,
                    )
                    * HD**-0.5
                )
                query_pos = lax.broadcasted_iota(jnp.int32, (rows, keys), 0) + i * rows
                key_pos = lax.broadcasted_iota(jnp.int32, (rows, keys), 1)
                scores = jnp.where(key_pos <= query_pos, scores, -1e30)
                powers = jnp.exp(scores - jnp.max(scores, axis=-1, keepdims=True))
                shares = (powers / jnp.sum(powers, axis=-1, keepdims=True)).astype(BF16)
                mixed = jnp.dot(shares, proj_v[2, h, :keys, :], preferred_element_type=F32)
                att_v[i * rows : keys, h * HD : (h + 1) * HD] = mixed.astype(BF16)
        a_copy = pltpu.make_async_copy(att_v, attended_out, a_sem)
        a_copy.start()
        a_copy.wait()
        n_copy.wait()

    dma = pltpu.SemaphoreType.DMA
    return call(
        body,
        "qkv_attend",
        (
            jax.ShapeDtypeStruct((length, width), BF16),
            jax.ShapeDtypeStruct((length, cols), BF16),
        ),
        [
            pltpu.VMEM((seq, rows, width), BF16),
            pltpu.VMEM((3, width, cols), BF16),
            pltpu.VMEM((length, width), BF16),
            pltpu.VMEM((3, heads, length, HD), BF16),
            pltpu.VMEM((length, cols), BF16),
            pltpu.VMEM(scale_all.shape, F32),
            dma((seq,)),
            dma((dp,)),
            dma,
            dma,
            dma,
        ],
        2 * length * width * 3 * cols,
        2 * (length * width * 2 + 3 * width * cols),
        (*tokens, *pieces, scale_all),
    )


def mix_middle(attended, pieces, normed, mix_rates, dp, seq):
    length, inner = attended[0].shape
    part = pieces[0].shape[1]
    width = part * dp
    tile = min(512, width)
    step = 128

    def body(*refs):
        att_refs = refs[:seq]
        piece_refs = refs[seq : seq + dp]
        normed_ref, rates_ref, mid_out = refs[seq + dp : seq + dp + 3]
        att_v, w_v, normed_v, sum_v, mid_v, rates_v, a_sem, w_sem, n_sem, r_sem, m_sem = refs[seq + dp + 3 :]
        d = lax.axis_index("dp")
        copies = [
            pltpu.make_async_copy(att_refs[j], att_v.at[:, j * inner : (j + 1) * inner], a_sem.at[j])
            for j in range(seq)
        ]
        copies += [
            pltpu.make_async_copy(piece_refs[k], w_v.at[:, at(d ^ k, part)], w_sem.at[k]) for k in range(dp)
        ]
        late = [
            pltpu.make_async_copy(normed_ref, normed_v, n_sem),
            pltpu.make_async_copy(rates_ref, rates_v, r_sem),
        ]
        for c in copies + late:
            c.start()
        for c in copies:
            c.wait()

        @pl.loop(0, width // tile)
        def _(t):
            sum_v[:, at(t, tile)] = jnp.dot(att_v[...], w_v[:, at(t, tile)], preferred_element_type=F32)

        for c in late:
            c.wait()

        @pl.loop(0, length // step)
        def _(r):
            rows = at(r, step)
            normed_f = normed_v[rows, :].astype(F32)
            mixed = normed_f + rates_v[0:1, :] * (unit(sum_v[rows, :]) - normed_f)
            mid_v[rows, :] = unit(mixed).astype(BF16)

        m_copy = pltpu.make_async_copy(mid_v, mid_out, m_sem)
        m_copy.start()
        m_copy.wait()

    dma = pltpu.SemaphoreType.DMA
    return call(
        body,
        "mix_middle",
        jax.ShapeDtypeStruct((length, width), BF16),
        [
            pltpu.VMEM((length, inner * seq), BF16),
            pltpu.VMEM((inner * seq, width), BF16),
            pltpu.VMEM((length, width), BF16),
            pltpu.VMEM((length, width), F32),
            pltpu.VMEM((length, width), BF16),
            pltpu.VMEM(mix_rates.shape, F32),
            dma((seq,)),
            dma((dp,)),
            dma,
            dma,
            dma,
        ],
        2 * length * inner * seq * width,
        2 * (length * width * 2 + inner * seq * width),
        (*attended, *pieces, normed, mix_rates),
    )


def gate_up(middle, pieces, mlp_scales, dp):
    length, width = middle.shape
    units = mlp_scales.shape[1]
    part = width // dp
    tile = min(256, units)
    tiles = units // tile
    flat = [p for piece in pieces for p in piece]

    def body(*refs):
        mid_ref = refs[0]
        flat_refs = list(refs[1 : 1 + len(flat)])
        scales_ref, hid_out = refs[1 + len(flat) : 3 + len(flat)]
        mid_v, w_v, hid_v, scales_v, m_sem, w_sem, s_sem, h_sem = refs[3 + len(flat) :]
        d = lax.axis_index("dp")

        def copies(t):
            made, left = [], list(flat_refs)
            for k in range(dp):
                first = left.pop(0)
                second = left.pop(0) if len(pieces[k]) == 2 else None
                for c in range(2):
                    source = first.at[c] if second is None else (first if c == 0 else second)
                    made.append(
                        pltpu.make_async_copy(
                            source.at[:, at(t, tile)],
                            w_v.at[c, at(d ^ k, part), at(t, tile)],
                            w_sem.at[t],
                        )
                    )
            return made

        m_copy = pltpu.make_async_copy(mid_ref, mid_v, m_sem)
        s_copy = pltpu.make_async_copy(scales_ref, scales_v, s_sem)
        m_copy.start()
        s_copy.start()

        @pl.loop(0, tiles)
        def _(t):
            for c in copies(t):
                c.start()

        m_copy.wait()
        s_copy.wait()

        def out_copy(t):
            return pltpu.make_async_copy(hid_v.at[:, at(t, tile)], hid_out.at[:, at(t, tile)], h_sem.at[t])

        @pl.loop(0, tiles)
        def _(t):
            for c in copies(t):
                c.wait()
            cols = at(t, tile)
            gate = jnp.dot(mid_v[...], w_v[0, :, cols], preferred_element_type=F32) * scales_v[0:1, cols]
            up = jnp.dot(mid_v[...], w_v[1, :, cols], preferred_element_type=F32) * scales_v[1:2, cols]
            hid_v[:, cols] = (gate / (1.0 + jnp.exp(-gate)) * up).astype(BF16)
            out_copy(t).start()

        @pl.loop(0, tiles)
        def _(t):
            out_copy(t).wait()

    dma = pltpu.SemaphoreType.DMA
    return call(
        body,
        "gate_up",
        jax.ShapeDtypeStruct((length, units), BF16),
        [
            pltpu.VMEM((length, width), BF16),
            pltpu.VMEM((2, width, units), BF16),
            pltpu.VMEM((length, units), BF16),
            pltpu.VMEM(mlp_scales.shape, F32),
            dma,
            dma((tiles,)),
            dma,
            dma((tiles,)),
        ],
        4 * length * width * units,
        2 * (length * width + 2 * width * units + length * units),
        (middle, *flat, mlp_scales),
    )


def down(hidden, pieces, seq, name):
    length, units = hidden.shape
    rows = length // seq
    count = len(pieces)
    part = pieces[0][0].shape[1]
    flat = [p for piece in pieces for p in piece]

    def body(*refs):
        hid_ref = refs[0]
        flat_refs = list(refs[1 : 1 + len(flat)])
        outs = refs[1 + len(flat) : 1 + len(flat) + seq]
        hid_v, w_v, sum_v, own_v, far_v, h_sem, w_sem, o_sem = refs[1 + len(flat) + seq :]
        z = lax.axis_index("seq")
        h_copy = pltpu.make_async_copy(hid_ref, hid_v, h_sem)
        h_copy.start()
        w_copies, left = [], list(flat_refs)
        for i in range(count):
            lows, made = 0, []
            for _ in pieces[i]:
                source = left.pop(0)
                high = lows + source.shape[0]
                made.append(pltpu.make_async_copy(source, w_v.at[i, lows:high, :], w_sem.at[len(w_copies), len(made)]))
                lows = high
            w_copies.append(made)
        for made in w_copies:
            for c in made:
                c.start()
        h_copy.wait()
        for i in range(count):
            for c in w_copies[i]:
                c.wait()
            sum_v[...] = jnp.dot(hid_v[...], w_v[i], preferred_element_type=F32)
            cols = slice(i * part, (i + 1) * part)
            own_v[:, cols] = sum_v[at(z, rows), :]
            for j in range(1, seq):
                far_v[j - 1, :, cols] = sum_v[at(z ^ j, rows), :].astype(BF16)
        o_copies = [pltpu.make_async_copy(own_v, outs[0], o_sem.at[0])]
        o_copies += [pltpu.make_async_copy(far_v.at[j - 1], outs[j], o_sem.at[j]) for j in range(1, seq)]
        for c in o_copies:
            c.start()
        for c in o_copies:
            c.wait()

    dma = pltpu.SemaphoreType.DMA
    wide = count * part
    return call(
        body,
        name,
        (jax.ShapeDtypeStruct((rows, wide), F32),) + (jax.ShapeDtypeStruct((rows, wide), BF16),) * (seq - 1),
        [
            pltpu.VMEM((length, units), BF16),
            pltpu.VMEM((count, units, part), BF16),
            pltpu.VMEM((length, part), F32),
            pltpu.VMEM((rows, wide), F32),
            pltpu.VMEM((seq - 1, rows, wide), BF16),
            dma,
            dma((count, 2)),
            dma((seq,)),
        ],
        2 * length * units * wide,
        2 * (length * units + units * wide + length * wide),
        (hidden, *flat),
    )


def finish(chunks, middle, mix_rates, dp, seq):
    width = middle.shape[1]
    rows = middle.shape[0] // seq
    part = width // dp
    arrays = [a for _, own, far in chunks for a in (own, *far)]

    def body(*refs):
        array_refs = list(refs[: len(arrays)])
        mid_ref, rates_ref, out_ref = refs[len(arrays) : len(arrays) + 3]
        rest = list(refs[len(arrays) + 3 :])
        own_v = [rest.pop(0) for _ in chunks]
        far_v = [rest.pop(0) for _ in chunks]
        feed_v, mid_v, rates_v, res_v, sem, m_sem, r_sem, out_sem = rest
        d, z = lax.axis_index("dp"), lax.axis_index("seq")
        copies = []
        for n in range(len(chunks)):
            for j in range(seq):
                target = own_v[n] if j == 0 else far_v[n].at[j - 1]
                copies.append(pltpu.make_async_copy(array_refs.pop(0), target, sem.at[n, j]))
        copies.append(pltpu.make_async_copy(mid_ref.at[at(z, rows), :], mid_v, m_sem))
        copies.append(pltpu.make_async_copy(rates_ref, rates_v, r_sem))
        for c in copies:
            c.start()
        for c in copies:
            c.wait()
        for n, (first, own, _) in enumerate(chunks):
            for i in range(own.shape[1] // part):
                cols = slice(i * part, (i + 1) * part)
                total = own_v[n][:, cols]
                for j in range(1, seq):
                    total = total + far_v[n][j - 1, :, cols].astype(F32)
                feed_v[:, at(d ^ (first + i), part)] = total
        middle_f = mid_v[...].astype(F32)
        mixed = middle_f + rates_v[1:2, :] * (unit(feed_v[...]) - middle_f)
        res_v[...] = unit(mixed).astype(BF16)
        copy = pltpu.make_async_copy(res_v, out_ref, out_sem)
        copy.start()
        copy.wait()

    dma = pltpu.SemaphoreType.DMA
    return call(
        body,
        "finish",
        jax.ShapeDtypeStruct((rows, width), BF16),
        [pltpu.VMEM(own.shape, F32) for _, own, _ in chunks]
        + [pltpu.VMEM((seq - 1,) + own.shape, BF16) for _, own, _ in chunks]
        + [
            pltpu.VMEM((rows, width), F32),
            pltpu.VMEM((rows, width), BF16),
            pltpu.VMEM(mix_rates.shape, F32),
            pltpu.VMEM((rows, width), BF16),
            dma((len(chunks), seq)),
            dma,
            dma,
            dma,
        ],
        20 * rows * width,
        2 * rows * width * 8,
        (*arrays, middle, mix_rates),
    )


def on_device(
    dp, seq, tokens, qkv_weight, qk_scale, out_weight, mix_rates, gate_up_weight, mlp_scales, down_weight
):
    all_tokens = gather_line(tokens[0], "seq", seq)
    qkv = [p[0] for p in gather_plane(qkv_weight, "dp", dp, None)]
    out_rows = gather_line(out_weight, "seq", seq)
    out = [p[0] for p in gather_plane(jnp.concatenate(out_rows, axis=0), "dp", dp, None)]
    gate_up_pieces = gather_plane(gate_up_weight, "dp", dp, lambda a: (a[0], a[1]))
    half = down_weight.shape[0] // 2
    down_pieces = gather_plane(down_weight, "dp", dp, lambda a: (a[:half], a[half:]))

    normed, attended = qkv_attend(all_tokens, qkv, qk_scale.reshape(-1, HD), dp, seq)
    all_attended = gather_line(attended, "seq", seq)
    middle = mix_middle(all_attended, out, normed, mix_rates, dp, seq)
    hidden = gate_up(middle, gate_up_pieces, mlp_scales, dp)
    chunks = []
    first = 0
    for n, size in enumerate((dp // 4, dp // 2, dp // 4)):
        own, *far = down(hidden, down_pieces[first : first + size], seq, f"down_{n}")
        far = [flip(a, "seq", j, seq) for j, a in enumerate(far, 1)]
        chunks.append((first, own, far))
        first += size
    return finish(chunks, middle, mix_rates, dp, seq)[None]


def solution(mesh):
    return jax.shard_map(
        functools.partial(on_device, mesh.shape["dp"], mesh.shape["seq"]),
        mesh=mesh,
        in_specs=(
            P("dp", "seq", None),
            P(None, "dp", "seq"),
            P(),
            P("seq", "dp"),
            P(),
            P(None, "dp", "seq"),
            P(None, "seq"),
            P("seq", "dp"),
        ),
        out_specs=P("dp", "seq", None),
        check_vma=False,
    )
```
